256 devices in a mesh: grp: 16 (over z, core), tp: 16 (over y, x).
Axes of the slice: x: 4, y: 4, z: 8, core: 2. Of those that a mesh axis runs over, the one named last changes fastest.
Arguments:
- window_queries: bfloat16 [512, 16384], P('grp', 'tp'), parts along dimension 0, may hold values from -64 to 64
- key_rows: bfloat16 [16, 262144, 128], P('tp', 'grp'), parts along dimension 1, may hold values from -16 to 16
- value_rows: bfloat16 [16, 262144, 128], P('tp', 'grp'), parts along dimension 1, may hold values from -6 to 6
- kept: int32 [8, 32768], P(None, 'grp'), parts along dimension 1, may hold values from 0 to 32735, as said below
Outputs:
- window_out: bfloat16 [512, 16384], P('grp', 'tp'), parts along dimension 0
- kept_keys: bfloat16 [16, 8, 4096, 128], P('tp', None, 'grp'), parts along dimension 2
- kept_values: bfloat16 [16, 8, 4096, 128], P('tp', None, 'grp'), parts along dimension 2
- kept_votes: bfloat16 [16, 128, 256], P('tp', 'grp'), parts along dimension 1
The draws below stay inside these ranges and needn't reach their ends.
There are 16 independent parts, one for each index of `grp`. The reference program is written for one: setup_inputs(seed, part) draws one part's arguments, and reference() takes and returns one part's arrays. A program takes and returns all parts, laid end to end along the dimension named above; each array names one. Nothing has to cross between parts.
Inputs may be any that keep to these rules, and one draw needn't show every extreme that they name: `kept`: each row lists 2048 distinct positions in ascending order, all below 32736; the first 1024 lie below 16384, the rest at or above it. For every head and half, at most 128 of its positions belong to one owner (owner (p // 128) mod 16), and some owner gets exactly 128.
All inputs are finite; a program needn't handle non-finite values.
Results may differ from the reference program's by a relative error of at most 0.005.
Values may be sent and summed in bfloat16 or wider, within the bound.
A program may use at most 128 MiB of HBM per device.

```python
import jax
import jax.numpy as jnp
from jax import lax

HQ = 128
KVH = 8
DH = 128
SEQ = 32768
WIN = 32
KEEP = 2048
OWNER_BLOCK = 128
OWNERS = 16
CAP = 128


def paired_draw(key):
    root_key = jax.random.fold_in(key, 11)
    key_cube = jax.random.normal(jax.random.fold_in(root_key, 1), (KVH, SEQ, DH), jnp.float32)
    queries = jax.random.normal(jax.random.fold_in(root_key, 2), (WIN, KVH, HQ // KVH, DH), jnp.float32)
    return (jnp.clip(key_cube, -16.0, 16.0), jnp.clip(queries, -64.0, 64.0))


def draw_key_rows(key, part):
    key_cube, queries = paired_draw(key)
    return key_cube.reshape(2 * KVH, SEQ // 2, DH).astype(jnp.bfloat16)


def draw_window_queries(key, part):
    key_cube, queries = paired_draw(key)
    return queries.reshape(WIN, HQ * DH).astype(jnp.bfloat16)


def draw_kept(key, part):
    half_len = SEQ // 2
    per_half = KEEP // 2
    capacity = CAP
    prefix = SEQ - WIN
    span = half_len // OWNERS
    root_key = jax.random.fold_in(key, 31)

    def one_list(row_key, side):
        order_key, delta_key, pick_key = jax.random.split(row_key, 3)
        ranking = jax.random.permutation(order_key, OWNERS).astype(jnp.int32)
        slot_of = jnp.arange(OWNERS, dtype=jnp.int32)
        pair_of = jnp.clip((slot_of - 3) // 2, 0, OWNERS - 1)
        deltas = jax.random.randint(delta_key, (OWNERS,), 0, capacity // 4)
        sign_of = jnp.where(slot_of < 3, 0, jnp.where((slot_of - 3) % 2 == 0, 1, -1))
        lonely = jnp.logical_and(slot_of == OWNERS - 1, (OWNERS - 3) % 2 == 1)
        sign_of = jnp.where(lonely, 0, sign_of)
        by_rank = capacity // 2 + sign_of * deltas[pair_of]
        by_rank = jnp.where(slot_of == 0, capacity, jnp.where(slot_of < 3, capacity // 4, by_rank))
        counts = jnp.zeros((OWNERS,), jnp.int32).at[ranking].set(by_rank.astype(jnp.int32))
        offsets = jnp.arange(half_len, dtype=jnp.int32)
        positions = side * half_len + offsets
        owner_of = positions // OWNER_BLOCK % OWNERS
        shuffle = jax.random.permutation(pick_key, half_len).astype(jnp.int32) + 1
        shuffle = jnp.where(positions >= prefix, shuffle + half_len, shuffle)
        boundary = jnp.where(side == 0, half_len - 1, half_len)
        shuffle = jnp.where(positions == boundary, 0, shuffle)
        sort_key = owner_of * (2 * half_len + 2) + shuffle
        order = jnp.argsort(sort_key)
        owner_sorted = owner_of[order]
        rank_sorted = offsets - owner_sorted * span
        take_sorted = rank_sorted < counts[owner_sorted]
        chosen_mask = jnp.zeros((half_len,), jnp.bool_).at[order].set(take_sorted)
        chosen = jnp.nonzero(chosen_mask, size=per_half)[0].astype(jnp.int32)
        return chosen + side * half_len
    row_keys = jax.random.split(root_key, 2 * KVH)
    sides = jnp.arange(2 * KVH, dtype=jnp.int32) % 2
    lists = jax.vmap(one_list)(row_keys, sides)
    return lists.reshape(KVH, KEEP)


def levels(stream_key, extent, shards, least, largest):
    def one(dim, shards_of):
        draws = jax.random.uniform(jax.random.fold_in(jax.random.fold_in(stream_key, 6), dim), (shards_of,), jnp.float32, least / len(shards), largest / len(shards))
        return jnp.repeat(jnp.exp(draws), extent[dim] // shards_of).reshape((-1,) + (1,) * (len(extent) - dim - 1))

    gain = one(*shards[0])
    for cut in shards[1:]:
        gain = gain * one(*cut)
    return gain


def scatter_about(stream_key, dims, deviation, most, cuts=(), held_as=jnp.bfloat16):
    values = jax.random.normal(stream_key, dims, jnp.float32) * deviation
    if len(cuts) > 0:
        values = levels(stream_key, dims, cuts, -0.22, 0.18) * values
    return jnp.clip(values, min=-most, max=most).astype(held_as)


def setup_inputs(seed: int = 0, part: int = 0) -> dict:
    arg_keys = jax.random.split(jax.random.key(seed), 5)
    part_keys = jax.random.split(jax.random.fold_in(arg_keys[4], part), 5)
    return {
        "window_queries": draw_window_queries(jax.random.fold_in(jax.random.fold_in(arg_keys[4], part), 71), part),
        "key_rows": draw_key_rows(jax.random.fold_in(jax.random.fold_in(arg_keys[4], part), 71), part),
        "value_rows": scatter_about(part_keys[2], (2 * KVH, SEQ // 2, DH), 1.0, 6.0, ((0, 16),)),
        "kept": draw_kept(jax.random.fold_in(jax.random.fold_in(arg_keys[4], part), 71), part),
    }


masked_score = -1.0e30


def reference(window_queries, key_rows, value_rows, kept):
    key_cube = key_rows.reshape(KVH, SEQ, DH)
    value_cube = value_rows.reshape(KVH, SEQ, DH)
    group_size = HQ // KVH
    queries = window_queries.reshape(WIN, KVH, group_size, DH).transpose(1, 2, 0, 3)
    prefix = SEQ - WIN
    factor = prefix / (7.0 * group_size * WIN)

    def per_head(element):
        query_set, key_set, value_set = element
        scores = jnp.einsum("gwd,pd->gwp", query_set.astype(jnp.float32), key_set.astype(jnp.float32)) * (DH ** -0.5)
        query_pos = prefix + jnp.arange(WIN, dtype=jnp.int32)[None, :, None]
        key_pos = jnp.arange(SEQ, dtype=jnp.int32)[None, None, :]
        scores = jnp.where(key_pos <= query_pos, scores, masked_score)
        row_max = jnp.max(scores, axis=-1, keepdims=True)
        expo = jnp.exp(scores - row_max)
        row_sum = jnp.sum(expo, axis=-1, keepdims=True)
        weights = expo / row_sum
        output = jnp.einsum("gwp,pd->gwd", weights.astype(jnp.bfloat16).astype(jnp.float32), value_set.astype(jnp.float32))
        vote_sum = jnp.sum(weights[:, :, :prefix], axis=(0, 1))
        padded = jnp.pad(vote_sum, (3, 3 + WIN))
        pooled = padded[0:SEQ]
        for offset in range(1, 7):
            pooled = pooled + padded[offset:offset + SEQ]
        return output, pooled * factor

    outputs, pooled = lax.map(per_head, (queries, key_cube, value_cube))
    window_out = outputs.transpose(2, 0, 1, 3).reshape(WIN, HQ * DH).astype(jnp.bfloat16)

    per_half = KEEP // 2
    positions = kept.reshape(KVH, 2, per_half).astype(jnp.int32)
    owner_of = (positions // OWNER_BLOCK) % OWNERS
    one_hot = (owner_of[..., None] == jnp.arange(OWNERS, dtype=jnp.int32)).astype(jnp.int32)
    rank_of = jnp.sum(jnp.cumsum(one_hot, axis=2) * one_hot, axis=3) - 1
    side_of = jnp.arange(2, dtype=jnp.int32)[None, :, None]
    slot_of = (side_of * CAP + rank_of).astype(jnp.int32)
    head_index = jnp.broadcast_to(jnp.arange(KVH, dtype=jnp.int32)[:, None, None], positions.shape)
    kept_keys = jnp.zeros((OWNERS, KVH, 2 * CAP, DH), jnp.bfloat16).at[owner_of, head_index, slot_of].set(key_cube[head_index, positions])
    kept_values = jnp.zeros((OWNERS, KVH, 2 * CAP, DH), jnp.bfloat16).at[owner_of, head_index, slot_of].set(value_cube[head_index, positions])
    kept_votes = jnp.zeros((OWNERS, KVH, 2 * CAP), jnp.bfloat16).at[owner_of, head_index, slot_of].set(pooled[head_index, positions].astype(jnp.bfloat16))
    return window_out, kept_keys, kept_values, kept_votes
```

```python
import functools

import jax
import jax.numpy as jnp
from jax import lax
from jax.experimental import pallas as pl
from jax.experimental.pallas import tpu as pltpu
from jax.sharding import PartitionSpec as P

SEQ = 32768
WIN = 32
HALF = 16384
CHUNKS = 8
OWNERS = 16
BLOCK = 128
ROWS = 256
CHUNK = OWNERS * BLOCK
SCALE = 1.4426950408889634 / 128.0**0.5
FACTOR = (SEQ - WIN) / (7.0 * 16 * WIN)
MASKED = -1e30
F32 = jnp.float32
BF16 = jnp.bfloat16
MESH = pl.DeviceIdType.MESH


def contract_last(a, b):
    return lax.dot_general(a, b, (((1,), (1,)), ((), ())), preferred_element_type=F32)


def mm(a, b):
    return jnp.dot(a, b, preferred_element_type=F32)


def iota(shape, dim):
    return lax.broadcasted_iota(jnp.int32, shape, dim)


def as_bf16(condition):
    return jnp.where(condition, 1.0, 0.0).astype(BF16)


def kernel(
    q_ref, k_hbm, v_hbm, kept_ref,
    wout_ref, kk_ref, vv_ref, vout_ref,
    kv, vt, ebuf, s_a, s_b, q_t, oacc, orecv, mrun, st_send, st_recv,
    slot_of, in_block, band, slot_hot, sendbuf, khalo, vext, vsend, vrecv, vstage,
    load_k, load_v, own_sem, a2a_send, a2a_recv, q_sem, halo_sem, st_sem, o_sem, vote_send, vote_recv,
):
    me = lax.axis_index("tp")
    grp = lax.axis_index("grp")
    side = me % 2
    head = me // 2
    mate = me + 1 - 2 * side

    def peer(rel):
        return (me + rel) % OWNERS

    def remote(src, dst, send, recv, to):
        return pltpu.make_async_remote_copy(
            src_ref=src, dst_ref=dst, send_sem=send, recv_sem=recv, device_id=(grp, to), device_id_type=MESH
        )

    def k_load(k):
        return pltpu.make_async_copy(k_hbm.at[k], kv.at[:, k, :, pl.ds(0, 128)], load_k.at[k])

    def v_load(k):
        return pltpu.make_async_copy(v_hbm.at[k], kv.at[:, k, :, pl.ds(128, 128)], load_v.at[k])

    barrier = pltpu.get_barrier_semaphore()
    for rel in range(1, OWNERS):
        pl.semaphore_signal(barrier, inc=1, device_id=(grp, peer(rel)), device_id_type=MESH)
    for k in range(CHUNKS):
        k_load(k).start()
        v_load(k).start()

    queries = jnp.concatenate([q_ref[:, a * 128 : (a + 1) * 128] for a in range(8)], axis=0)
    q_t[0] = queries.astype(F32).T.astype(BF16)

    mine = jnp.sum(jnp.where(iota((8, 2048), 0) == head, kept_ref[...], 0), axis=0, keepdims=True)
    pos = jnp.where(side == 0, mine[:, :1024], mine[:, 1024:] - HALF)
    blk = pos // BLOCK
    lane = pos % BLOCK
    hot_block = as_bf16(iota((128, 1024), 0) == blk)
    hot_lane = as_bf16(iota((128, 1024), 0) == lane)
    in_block[...] = hot_block
    away = iota((384, 1024), 0) - 128 - lane
    band[...] = as_bf16((away <= 3) & (away >= -3))
    mask = contract_last(hot_block, hot_lane)
    mask16 = mask.astype(BF16)
    r, c = iota((128, 128), 0), iota((128, 128), 1)
    before = mm(mask16, as_bf16(r < c))
    same = mm(as_bf16((c < r) & ((r - c) % OWNERS == 0)), mask16).astype(BF16)
    ahead = mm(same, jnp.ones((128, 128), BF16))
    slots = jnp.where(mask > 0.5, before + ahead, -1.0)
    slot_of[...] = slots
    picked = mm(slots.astype(BF16), hot_lane)
    slot_i = jnp.sum(jnp.where(hot_block > 0.5, picked, 0.0), axis=0, keepdims=True)
    slot_hot[...] = as_bf16(iota((128, 1024), 0).astype(F32) == slot_i)

    window_of = iota((WIN, ROWS), 1) % WIN
    hidden_row = iota((WIN, ROWS), 0) > window_of
    oacc[...] = jnp.zeros_like(oacc)

    def scores(k, group, s_ref):
        keys = kv[:, k, :, 0:128].reshape(CHUNK, 128)
        s = mm(keys, q_t[group])
        hide = jnp.logical_and(hidden_row, jnp.logical_and(side == 1, k == CHUNKS - 1))
        last = jnp.where(hide, MASKED, s[CHUNK - WIN :])
        s_ref[0 : CHUNK - WIN, :] = s[: CHUNK - WIN]
        s_ref[CHUNK - WIN :, :] = last
        return jnp.maximum(
            jnp.max(s[: CHUNK - WIN], axis=0, keepdims=True), jnp.max(last, axis=0, keepdims=True)
        )

    def transpose_values(k):
        for o in range(OWNERS):
            vt[k, 0:128, o * 128 : (o + 1) * 128] = kv[o, k, :, 128:256].T
        vt[k, 128:144, :] = jnp.ones((16, CHUNK), BF16)

    def weigh(k, group, s_ref, old, new):
        u = group * CHUNKS + k
        shift = new * SCALE
        e = jnp.exp2(s_ref[...] * SCALE - shift).astype(BF16)
        ebuf[u] = e
        alpha = jnp.exp2(old * SCALE - shift)
        mrun[u] = jnp.broadcast_to(new, (8, ROWS))
        oacc[group] = oacc[group] * alpha + mm(vt[k], e)

    def attend(group):
        def ready(k):
            if group == 0:
                k_load(k).wait()
                v_load(k).wait()

        def step(t, carry):
            m_old, mx = carry
            k0, k1 = 2 * t, 2 * t + 1
            ready(k1)
            if group == 0:
                transpose_values(k0)
                transpose_values(k1)
            m_new = jnp.maximum(m_old, mx)
            mx1 = scores(k1, group, s_b)
            weigh(k0, group, s_a, m_old, m_new)
            m_last = jnp.maximum(m_new, mx1)
            if group == 0:
                @pl.when(t < CHUNKS // 2 - 1)
                def _():
                    ready(k0 + 2)
            k2 = jnp.minimum(k0 + 2, CHUNKS - 1)
            mx2 = scores(k2, group, s_a)
            weigh(k1, group, s_b, m_new, m_last)
            return m_last, mx2

        ready(0)
        mx = scores(0, group, s_a)
        m, unused = lax.fori_loop(0, CHUNKS // 2, step, (jnp.full((1, ROWS), MASKED, F32), mx))
        st_send[group, 0:8, :] = jnp.broadcast_to(m, (8, ROWS))
        st_send[group, 8:16, :] = oacc[group, 128:136, :]
        return m

    m_own = attend(0)

    def pick(rel, unused):
        o = peer(rel)
        slot_row = iota((128, 128), 0).astype(F32)
        hot = jnp.concatenate(
            [as_bf16(slot_row == slot_of[pl.ds(16 * k + o, 1), :]) for k in range(CHUNKS)], axis=1
        )
        rows = mm(hot, kv[o].reshape(CHUNKS * 128, 256)).astype(BF16)
        sendbuf[o, 0] = rows[:, 0:128]
        sendbuf[o, 1] = rows[:, 128:256]
        return unused

    lax.fori_loop(0, OWNERS, pick, 0)

    pl.semaphore_wait(barrier, OWNERS - 1)
    q_copy = remote(q_t.at[0], q_t.at[1], q_sem.at[0], q_sem.at[1], mate)
    q_copy.start()
    edge_owner = 15 - 15 * side
    edge_chunk = 7 - 7 * side
    halo_copy = remote(
        kv.at[edge_owner, edge_chunk, :, pl.ds(0, 128)], khalo, halo_sem.at[0], halo_sem.at[1], mate
    )
    halo_copy.start()
    own_stat = remote(st_send.at[0], st_recv.at[0], st_sem.at[0], st_sem.at[1], mate)
    own_stat.start()

    def row_copies(rel):
        o = peer(rel)
        return [
            remote(
                sendbuf.at[o, n],
                out.at[head, pl.ds(side * 128, 128), :],
                a2a_send.at[n, rel],
                a2a_recv.at[n, rel],
                o,
            )
            for n, out in enumerate((kk_ref, vv_ref))
        ]

    def local_copies():
        return [
            pltpu.make_async_copy(sendbuf.at[me, n], out.at[head, pl.ds(side * 128, 128), :], own_sem.at[n])
            for n, out in enumerate((kk_ref, vv_ref))
        ]

    for rel in range(1, OWNERS):
        for copy in row_copies(rel):
            copy.start()
    for copy in local_copies():
        copy.start()

    q_copy.wait()
    m_mate = attend(1)
    mate_stat = remote(st_send.at[1], st_recv.at[1], st_sem.at[2], st_sem.at[3], mate)
    mate_stat.start()
    out_copy = remote(oacc.at[1], orecv, o_sem.at[0], o_sem.at[1], mate)
    out_copy.start()
    halo_copy.wait()
    s_halo = [mm(khalo[...], q_t[group]) for group in range(2)]
    own_stat.wait()
    mate_stat.wait()

    m_here = (m_own, m_mate)
    merged = []
    for group in range(2):
        m_there = st_recv[1 - group, 0:1, :]
        l_there = st_recv[1 - group, 8:9, :]
        m_all = jnp.maximum(m_here[group], m_there)
        here = jnp.exp2((m_here[group] - m_all) * SCALE)
        there = jnp.exp2((m_there - m_all) * SCALE)
        l_all = st_send[group, 8:9, :] * here + l_there * there
        merged.append((m_all, here, there, 1.0 / l_all))

    row_id = iota((16, ROWS), 0)

    def pieces(w):
        hi = w.astype(BF16).astype(F32)
        mid = (w - hi).astype(BF16).astype(F32)
        return jnp.where(row_id == 0, hi, jnp.where(row_id == 1, mid, 0.0)).astype(BF16)

    def tally(k, unused):
        total = jnp.zeros((16, CHUNK), F32)
        for group in range(2):
            m_all, here, there, inv = merged[group]
            u = group * CHUNKS + k
            w = jnp.exp2((mrun[u, 0:1, :] - m_all) * SCALE) * inv
            total = total + contract_last(pieces(w), ebuf[u])
        row = total[0:1, :] + total[1:2, :]
        for o in range(OWNERS):
            vext[pl.ds(8 + 16 * k + o, 1), :] = row[:, o * 128 : (o + 1) * 128]
        return unused

    lax.fori_loop(0, CHUNKS, tally, 0)
    halo_votes = jnp.zeros((16, 128), F32)
    for group in range(2):
        m_all, here, there, inv = merged[group]
        e = jnp.exp2(s_halo[group] * SCALE - m_all * SCALE).astype(BF16)
        halo_votes = halo_votes + contract_last(pieces(inv), e)
    halo_row = halo_votes[0:1, :] + halo_votes[1:2, :]
    vext[7:8, :] = jnp.where(side == 1, halo_row, 0.0)
    vext[136:137, :] = jnp.where(side == 0, halo_row, 0.0)
    cut = jnp.logical_and(iota((1, 128), 1) >= 128 - WIN, side == 1)
    vext[135:136, :] = jnp.where(cut, 0.0, vext[135:136, :])

    spread = jnp.concatenate([vext[7:135, :], vext[8:136, :], vext[9:137, :]], axis=1)
    hi = spread.astype(BF16)
    lo = (spread - hi.astype(F32)).astype(BF16)
    pooled = mm(hi, band[...]) + mm(lo, band[...])
    value = jnp.sum(jnp.where(in_block[...] > 0.5, pooled, 0.0), axis=0, keepdims=True) * FACTOR
    by_owner = jnp.where(iota((16, 1024), 0) == blk % OWNERS, value, 0.0).astype(BF16)
    placed = contract_last(by_owner, slot_hot[...])
    for o in range(OWNERS):
        vsend[o] = jnp.broadcast_to(placed[o : o + 1, :], (8, 128))

    def vote_copy(rel):
        return remote(vsend.at[peer(rel)], vrecv.at[me], vote_send.at[rel], vote_recv.at[rel], peer(rel))

    for rel in range(1, OWNERS):
        vote_copy(rel).start()
    vrecv[me] = vsend[me]

    out_copy.wait()
    m_all, here, there, inv = merged[0]
    merged_out = (oacc[0, 0:128, :] * here + orecv[0:128, :] * there) * inv
    by_row = merged_out.T.astype(BF16)
    for a in range(8):
        wout_ref[:, a * 128 : (a + 1) * 128] = by_row[a * WIN : (a + 1) * WIN, :]

    for copy in local_copies():
        copy.wait()
    for rel in range(1, OWNERS):
        for copy in row_copies(rel):
            copy.wait()
    for rel in range(1, OWNERS):
        remote(
            vsend.at[peer(rel)], vrecv.at[peer(OWNERS - rel)], vote_send.at[rel], vote_recv.at[rel], peer(rel)
        ).wait()
    for t in range(OWNERS):
        vstage[t // 2 : t // 2 + 1, (t % 2) * 128 : (t % 2) * 128 + 128] = vrecv[t, 0:1, :]
    vout_ref[...] = vstage[...].astype(BF16)


def on_device(window_queries, key_rows, value_rows, kept):
    vmem = pl.BlockSpec(memory_space=pltpu.VMEM)
    hbm = pl.BlockSpec(memory_space=pltpu.HBM)
    dma = pltpu.SemaphoreType.DMA
    shaped = (CHUNKS, OWNERS, BLOCK, 128)
    wout, kk, vv, votes = pl.pallas_call(
        kernel,
        out_shape=(
            jax.ShapeDtypeStruct((WIN, 1024), BF16),
            jax.ShapeDtypeStruct((8, 256, 128), BF16),
            jax.ShapeDtypeStruct((8, 256, 128), BF16),
            jax.ShapeDtypeStruct((8, 256), BF16),
        ),
        in_specs=[vmem, hbm, hbm, vmem],
        out_specs=(vmem, hbm, hbm, vmem),
        scratch_shapes=[
            pltpu.VMEM((OWNERS, CHUNKS, BLOCK, 256), BF16),
            pltpu.VMEM((CHUNKS, 144, CHUNK), BF16),
            pltpu.VMEM((2 * CHUNKS, CHUNK, ROWS), BF16),
            pltpu.VMEM((CHUNK, ROWS), F32),
            pltpu.VMEM((CHUNK, ROWS), F32),
            pltpu.VMEM((2, 128, ROWS), BF16),
            pltpu.VMEM((2, 144, ROWS), F32),
            pltpu.VMEM((144, ROWS), F32),
            pltpu.VMEM((2 * CHUNKS, 8, ROWS), F32),
            pltpu.VMEM((2, 16, ROWS), F32),
            pltpu.VMEM((2, 16, ROWS), F32),
            pltpu.VMEM((128, 128), F32),
            pltpu.VMEM((128, 1024), BF16),
            pltpu.VMEM((384, 1024), BF16),
            pltpu.VMEM((128, 1024), BF16),
            pltpu.VMEM((OWNERS, 2, 128, 128), BF16),
            pltpu.VMEM((128, 128), BF16),
            pltpu.VMEM((144, 128), F32),
            pltpu.VMEM((OWNERS, 8, 128), F32),
            pltpu.VMEM((OWNERS, 8, 128), F32),
            pltpu.VMEM((8, 256), F32),
            dma((CHUNKS,)),
            dma((CHUNKS,)),
            dma((2,)),
            dma((2, OWNERS)),
            dma((2, OWNERS)),
            dma((2,)),
            dma((2,)),
            dma((4,)),
            dma((2,)),
            dma((OWNERS,)),
            dma((OWNERS,)),
        ],
        compiler_params=pltpu.CompilerParams(
            collective_id=0, has_side_effects=True, vmem_limit_bytes=60 * 1024 * 1024
        ),
    )(window_queries, key_rows.reshape(shaped), value_rows.reshape(shaped), kept)
    return (wout, kk[None], vv[None], votes[None])


def solution(mesh):
    return jax.shard_map(
        on_device,
        mesh=mesh,
        in_specs=(P("grp", "tp"), P("tp", "grp", None), P("tp", "grp", None), P(None, "grp")),
        out_specs=(
            P("grp", "tp"),
            P("tp", None, "grp", None),
            P("tp", None, "grp", None),
            P("tp", "grp", None),
        ),
        check_vma=False,
    )
```

```python
import functools

import jax
import jax.numpy as jnp
from jax import lax
from jax.experimental import pallas as pl
from jax.experimental.pallas import tpu as pltpu
from jax.sharding import PartitionSpec as P

SEQ = 32768
WIN = 32
HALF = 16384
SPLIT = 1
FRONT = 2
CHUNKS = 8
OWNERS = 16
BLOCK = 128
ROWS = 256
CHUNK = OWNERS * BLOCK
SCALE = 1.4426950408889634 / 128.0**0.5
FACTOR = (SEQ - WIN) / (7.0 * 16 * WIN)
MASKED = -1e30
F32 = jnp.float32
BF16 = jnp.bfloat16
MESH = pl.DeviceIdType.MESH


def contract_last(a, b):
    return lax.dot_general(a, b, (((1,), (1,)), ((), ())), preferred_element_type=F32)


def mm(a, b):
    return jnp.dot(a, b, preferred_element_type=F32)


def iota(shape, dim):
    return lax.broadcasted_iota(jnp.int32, shape, dim)


def as_bf16(condition):
    return jnp.where(condition, 1.0, 0.0).astype(BF16)


def kernel(
    q_hbm, k_hbm, v_hbm, kept_hbm,
    wout_ref, kk_ref, vv_ref, vout_ref,
    q_ref, kept_ref, kv, vt, ebuf, s_a, s_b, q_t, oacc, orecv, mrun, st_send, st_recv,
    slot_of, in_block, band, slot_hot, sendbuf, khalo, vext, vsend, vrecv, vstage,
    load_in, load_k, load_v, own_sem, a2a_send, a2a_recv, q_sem, halo_sem, st_sem, o_sem, vote_send, vote_recv,
):
    me = lax.axis_index("tp")
    grp = lax.axis_index("grp")
    side = me % 2
    head = me // 2
    mate = me + 1 - 2 * side

    def peer(rel):
        return (me + rel) % OWNERS

    def remote(src, dst, send, recv, to):
        return pltpu.make_async_remote_copy(
            src_ref=src, dst_ref=dst, send_sem=send, recv_sem=recv, device_id=(grp, to), device_id_type=MESH
        )

    def k_load(k):
        return pltpu.make_async_copy(k_hbm.at[k], kv.at[:, k, :, pl.ds(0, 128)], load_k.at[k])

    def v_load(k):
        return pltpu.make_async_copy(v_hbm.at[k], kv.at[:, k, :, pl.ds(128, 128)], load_v.at[k])

    barrier = pltpu.get_barrier_semaphore()
    for rel in range(1, OWNERS):
        pl.semaphore_signal(barrier, inc=1, device_id=(grp, peer(rel)), device_id_type=MESH)
    kept_load = pltpu.make_async_copy(kept_hbm, kept_ref, load_in.at[0])
    q_load = pltpu.make_async_copy(q_hbm, q_ref, load_in.at[1])
    kept_load.start()
    q_load.start()
    for k in range(CHUNKS):
        k_load(k).start()
        v_load(k).start()
    kept_load.wait()
    q_load.wait()

    queries = jnp.concatenate([q_ref[:, a * 128 : (a + 1) * 128] for a in range(8)], axis=0)
    q_t[0] = queries.astype(F32).T.astype(BF16)

    mine = jnp.sum(jnp.where(iota((8, 2048), 0) == head, kept_ref[...], 0), axis=0, keepdims=True)
    pos = jnp.where(side == 0, mine[:, :1024], mine[:, 1024:] - HALF)
    blk = pos // BLOCK
    lane = pos % BLOCK
    hot_block = as_bf16(iota((128, 1024), 0) == blk)
    hot_lane = as_bf16(iota((128, 1024), 0) == lane)
    in_block[...] = hot_block
    away = iota((384, 1024), 0) - 128 - lane
    band[...] = as_bf16((away <= 3) & (away >= -3))
    mask = contract_last(hot_block, hot_lane)
    mask16 = mask.astype(BF16)
    r, c = iota((128, 128), 0), iota((128, 128), 1)
    before = mm(mask16, as_bf16(r < c))
    same = mm(as_bf16((c < r) & ((r - c) % OWNERS == 0)), mask16).astype(BF16)
    ahead = mm(same, jnp.ones((128, 128), BF16))
    slots = jnp.where(mask > 0.5, before + ahead, -1.0)
    slot_of[...] = slots
    picked = mm(slots.astype(BF16), hot_lane)
    slot_i = jnp.sum(jnp.where(hot_block > 0.5, picked, 0.0), axis=0, keepdims=True)
    slot_hot[...] = as_bf16(iota((128, 1024), 0).astype(F32) == slot_i)

    window_of = iota((WIN, ROWS), 1) % WIN
    hidden_row = iota((WIN, ROWS), 0) > window_of
    oacc[...] = jnp.zeros_like(oacc)

    def scores(k, group, s_ref):
        keys = kv[:, k, :, 0:128].reshape(CHUNK, 128)
        s = mm(keys, q_t[group])
        hide = jnp.logical_and(hidden_row, jnp.logical_and(side == 1, k == CHUNKS - 1))
        last = jnp.where(hide, MASKED, s[CHUNK - WIN :])
        s_ref[0 : CHUNK - WIN, :] = s[: CHUNK - WIN]
        s_ref[CHUNK - WIN :, :] = last
        return jnp.maximum(
            jnp.max(s[: CHUNK - WIN], axis=0, keepdims=True), jnp.max(last, axis=0, keepdims=True)
        )

    def transpose_values(k):
        for o in range(OWNERS):
            vt[k, 0:128, o * 128 : (o + 1) * 128] = kv[o, k, :, 128:256].T
        vt[k, 128:144, :] = jnp.ones((16, CHUNK), BF16)

    def weigh(k, group, s_ref, old, new):
        u = group * CHUNKS + k
        shift = new * SCALE
        e = jnp.exp2(s_ref[...] * SCALE - shift).astype(BF16)
        ebuf[u] = e
        alpha = jnp.exp2(old * SCALE - shift)
        mrun[u] = jnp.broadcast_to(new, (8, ROWS))
        oacc[group] = oacc[group] * alpha + mm(vt[k], e)

    def ready(k):
        k_load(k).wait()
        v_load(k).wait()

    def begin(group):
        if group == 0:
            ready(0)
        return jnp.full((1, ROWS), MASKED, F32), scores(0, group, s_a)

    def attend(group, first, last, carry, between):
        def step(t, carry):
            m_old, mx = carry
            k0, k1 = 2 * t, 2 * t + 1
            if group == 0:
                if first == 0:
                    ready(k1)
                transpose_values(k0)
                transpose_values(k1)
            between(t, 0)
            m_new = jnp.maximum(m_old, mx)
            mx1 = scores(k1, group, s_b)
            weigh(k0, group, s_a, m_old, m_new)
            m_last = jnp.maximum(m_new, mx1)
            if group == 0 and first == 0:
                ready(k0 + 2)
            between(t, 1)
            k2 = jnp.minimum(k0 + 2, CHUNKS - 1)
            mx2 = scores(k2, group, s_a)
            weigh(k1, group, s_b, m_new, m_last)
            return m_last, mx2

        return lax.fori_loop(first, last, step, carry)

    def finish(group, m):
        st_send[group, 0:8, :] = jnp.broadcast_to(m, (8, ROWS))
        st_send[group, 8:16, :] = oacc[group, 128:136, :]

    def row_copies(rel):
        o = peer(rel)
        return [
            remote(
                sendbuf.at[o, n],
                out.at[head, pl.ds(side * 128, 128), :],
                a2a_send.at[n, rel],
                a2a_recv.at[n, rel],
                o,
            )
            for n, out in enumerate((kk_ref, vv_ref))
        ]

    def send_rows(index):
        for copy in row_copies(index + 1):
            copy.start()

    def pick(rel, unused):
        o = peer(rel)
        slot_row = iota((128, 128), 0).astype(F32)
        hot = jnp.concatenate(
            [as_bf16(slot_row == slot_of[pl.ds(16 * k + o, 1), :]) for k in range(CHUNKS)], axis=1
        )
        rows = mm(hot, kv[o].reshape(CHUNKS * 128, 256)).astype(BF16)
        sendbuf[o, 0] = rows[:, 0:128]
        sendbuf[o, 1] = rows[:, 128:256]
        return unused

    def pick_four(t, unused):
        for n in range(4):
            pick(4 * t + n, 0)
        return unused

    carry = attend(0, 0, SPLIT, begin(0), lambda t, part: None)
    waited = 2 * SPLIT
    for k in range(waited + 1, CHUNKS):
        ready(k)
    lax.fori_loop(0, 4, pick_four, 0)
    pl.semaphore_wait(barrier, OWNERS - 1)
    q_copy = remote(q_t.at[0], q_t.at[1], q_sem.at[0], q_sem.at[1], mate)
    q_copy.start()
    edge_owner = 15 - 15 * side
    edge_chunk = 7 - 7 * side
    halo_copy = remote(
        kv.at[edge_owner, edge_chunk, :, pl.ds(0, 128)], khalo, halo_sem.at[0], halo_sem.at[1], mate
    )
    halo_copy.start()
    for n in range(FRONT):
        send_rows(n)

    def pace_own(t, part):
        send_rows(FRONT + 2 * (t - SPLIT) + part)

    m_own, unused = attend(0, SPLIT, CHUNKS // 2, carry, pace_own)
    finish(0, m_own)
    sent = FRONT + 2 * (CHUNKS // 2 - SPLIT)
    rest = OWNERS - 1 - sent

    def pace_mate(t, part):
        index = 2 * t + part

        @pl.when(index < rest)
        def _():
            send_rows(sent + index)

    own_stat = remote(st_send.at[0], st_recv.at[0], st_sem.at[0], st_sem.at[1], mate)
    own_stat.start()
    q_copy.wait()
    m_mate, unused = attend(1, 0, CHUNKS // 2, begin(1), pace_mate)
    finish(1, m_mate)
    mate_stat = remote(st_send.at[1], st_recv.at[1], st_sem.at[2], st_sem.at[3], mate)
    mate_stat.start()
    out_copy = remote(oacc.at[1], orecv, o_sem.at[0], o_sem.at[1], mate)
    out_copy.start()
    halo_copy.wait()
    s_halo = [mm(khalo[...], q_t[group]) for group in range(2)]
    own_stat.wait()
    mate_stat.wait()

    m_here = (m_own, m_mate)
    merged = []
    for group in range(2):
        m_there = st_recv[1 - group, 0:1, :]
        l_there = st_recv[1 - group, 8:9, :]
        m_all = jnp.maximum(m_here[group], m_there)
        here = jnp.exp2((m_here[group] - m_all) * SCALE)
        there = jnp.exp2((m_there - m_all) * SCALE)
        l_all = st_send[group, 8:9, :] * here + l_there * there
        merged.append((m_all, here, there, 1.0 / l_all))

    ones = jnp.ones((16, 128), BF16)

    def spread_rows(w):
        return jnp.broadcast_to(w, (16, ROWS)).astype(BF16)[None]

    def fold(parts):
        total = None
        for e, w in parts:
            product = e.reshape(e.shape[0] // 16, 16, ROWS) * w
            both = product[:, :, 0:128] + product[:, :, 128:256]
            total = both if total is None else total + both
        return contract_last(ones, total.reshape(-1, 128))[0:1, :]

    def tally(k, unused):
        parts = []
        for group in range(2):
            m_all, here, there, inv = merged[group]
            u = group * CHUNKS + k
            parts.append((ebuf[u], spread_rows(jnp.exp2((mrun[u, 0:1, :] - m_all) * SCALE) * inv)))
        row = fold(parts)
        for o in range(OWNERS):
            vext[pl.ds(8 + 16 * k + o, 1), :] = row[:, o * 128 : (o + 1) * 128]
        return unused

    lax.fori_loop(0, CHUNKS, tally, 0)
    parts = []
    for group in range(2):
        m_all, here, there, inv = merged[group]
        parts.append((jnp.exp2(s_halo[group] * SCALE - m_all * SCALE).astype(BF16), spread_rows(inv)))
    halo_row = fold(parts)
    vext[7:8, :] = jnp.where(side == 1, halo_row, 0.0)
    vext[136:137, :] = jnp.where(side == 0, halo_row, 0.0)
    cut = jnp.logical_and(iota((1, 128), 1) >= 128 - WIN, side == 1)
    vext[135:136, :] = jnp.where(cut, 0.0, vext[135:136, :])

    spread = jnp.concatenate([vext[7:135, :], vext[8:136, :], vext[9:137, :]], axis=1)
    hi = spread.astype(BF16)
    lo = (spread - hi.astype(F32)).astype(BF16)
    pooled = mm(hi, band[...]) + mm(lo, band[...])
    value = jnp.sum(jnp.where(in_block[...] > 0.5, pooled, 0.0), axis=0, keepdims=True) * FACTOR
    by_owner = jnp.where(iota((16, 1024), 0) == blk % OWNERS, value, 0.0).astype(BF16)
    placed = contract_last(by_owner, slot_hot[...])
    for o in range(OWNERS):
        vsend[o] = jnp.broadcast_to(placed[o : o + 1, :], (8, 128))

    def vote_copy(rel):
        return remote(vsend.at[peer(rel)], vrecv.at[me], vote_send.at[rel], vote_recv.at[rel], peer(rel))

    for rel in range(1, OWNERS):
        vote_copy(rel).start()
    vrecv[me] = vsend[me]
    for n, out in enumerate((kk_ref, vv_ref)):
        out[head, pl.ds(side * 128, 128), :] = sendbuf[me, n]

    out_copy.wait()
    m_all, here, there, inv = merged[0]
    merged_out = (oacc[0, 0:128, :] * here + orecv[0:128, :] * there) * inv
    by_row = merged_out.T.astype(BF16)
    for a in range(8):
        wout_ref[:, a * 128 : (a + 1) * 128] = by_row[a * WIN : (a + 1) * WIN, :]

    for rel in range(1, OWNERS):
        for copy in row_copies(rel):
            copy.wait()
    for rel in range(1, OWNERS):
        remote(
            vsend.at[peer(rel)], vrecv.at[peer(OWNERS - rel)], vote_send.at[rel], vote_recv.at[rel], peer(rel)
        ).wait()
    for t in range(OWNERS):
        vstage[t // 2 : t // 2 + 1, (t % 2) * 128 : (t % 2) * 128 + 128] = vrecv[t, 0:1, :]
    vout_ref[...] = vstage[...].astype(BF16)


def write_out(*refs):
    copies = [pltpu.make_async_copy(refs[n], refs[4 + n], refs[8].at[n]) for n in range(4)]
    for copy in copies:
        copy.start()
    for copy in copies:
        copy.wait()


def on_device(window_queries, key_rows, value_rows, kept):
    vmem = pl.BlockSpec(memory_space=pltpu.VMEM)
    hbm = pl.BlockSpec(memory_space=pltpu.HBM)
    dma = pltpu.SemaphoreType.DMA
    shaped = (CHUNKS, OWNERS, BLOCK, 128)
    inside = pl.pallas_call(
        kernel,
        out_shape=(
            pltpu.VMEM((WIN, 1024), BF16),
            pltpu.VMEM((8, 256, 128), BF16),
            pltpu.VMEM((8, 256, 128), BF16),
            pltpu.VMEM((8, 256), BF16),
        ),
        in_specs=[hbm] * 4,
        out_specs=(vmem,) * 4,
        scratch_shapes=[
            pltpu.VMEM((WIN, 1024), BF16),
            pltpu.VMEM((8, 2048), jnp.int32),
            pltpu.VMEM((OWNERS, CHUNKS, BLOCK, 256), BF16),
            pltpu.VMEM((CHUNKS, 144, CHUNK), BF16),
            pltpu.VMEM((2 * CHUNKS, CHUNK, ROWS), BF16),
            pltpu.VMEM((CHUNK, ROWS), F32),
            pltpu.VMEM((CHUNK, ROWS), F32),
            pltpu.VMEM((2, 128, ROWS), BF16),
            pltpu.VMEM((2, 144, ROWS), F32),
            pltpu.VMEM((144, ROWS), F32),
            pltpu.VMEM((2 * CHUNKS, 8, ROWS), F32),
            pltpu.VMEM((2, 16, ROWS), F32),
            pltpu.VMEM((2, 16, ROWS), F32),
            pltpu.VMEM((128, 128), F32),
            pltpu.VMEM((128, 1024), BF16),
            pltpu.VMEM((384, 1024), BF16),
            pltpu.VMEM((128, 1024), BF16),
            pltpu.VMEM((OWNERS, 2, 128, 128), BF16),
            pltpu.VMEM((128, 128), BF16),
            pltpu.VMEM((144, 128), F32),
            pltpu.VMEM((OWNERS, 8, 128), F32),
            pltpu.VMEM((OWNERS, 8, 128), F32),
            pltpu.VMEM((8, 256), F32),
            dma((2,)),
            dma((CHUNKS,)),
            dma((CHUNKS,)),
            dma((2,)),
            dma((2, OWNERS)),
            dma((2, OWNERS)),
            dma((2,)),
            dma((2,)),
            dma((4,)),
            dma((2,)),
            dma((OWNERS,)),
            dma((OWNERS,)),
        ],
        compiler_params=pltpu.CompilerParams(
            collective_id=0, has_side_effects=True, vmem_limit_bytes=56 * 1024 * 1024
        ),
    )(window_queries, key_rows.reshape(shaped), value_rows.reshape(shaped), kept)
    wout, kk, vv, votes = pl.pallas_call(
        write_out,
        out_shape=tuple(jax.ShapeDtypeStruct(a.shape, a.dtype) for a in inside),
        in_specs=[vmem] * 4,
        out_specs=(hbm,) * 4,
        scratch_shapes=[dma((4,))],
        compiler_params=pltpu.CompilerParams(vmem_limit_bytes=1024 * 1024),
    )(*inside)
    return (wout, kk[None], vv[None], votes[None])


def solution(mesh):
    return jax.shard_map(
        on_device,
        mesh=mesh,
        in_specs=(P("grp", "tp"), P("tp", "grp", None), P("tp", "grp", None), P(None, "grp")),
        out_specs=(
            P("grp", "tp"),
            P("tp", None, "grp", None),
            P("tp", None, "grp", None),
            P("tp", "grp", None),
        ),
        check_vma=False,
    )
```

```python
import functools

import jax
import jax.numpy as jnp
from jax import lax
from jax.experimental import pallas as pl
from jax.experimental.pallas import tpu as pltpu
from jax.sharding import PartitionSpec as P

SEQ = 32768
WIN = 32
HALF = 16384
SPLIT = 1
EARLY = (2, 4, 1, 3, 8, 6, 5, 7, 12, 10, 9, 11)
LATE = (14, 13, 15)
CHUNKS = 8
OWNERS = 16
BLOCK = 128
ROWS = 256
CHUNK = OWNERS * BLOCK
PIECE = 256
PIECES = CHUNK // PIECE
SCALE = 1.4426950408889634 / 128.0**0.5
FACTOR = (SEQ - WIN) / (7.0 * 16 * WIN)
MASKED = -1e30
F32 = jnp.float32
BF16 = jnp.bfloat16
MESH = pl.DeviceIdType.MESH


def contract_last(a, b):
    return lax.dot_general(a, b, (((1,), (1,)), ((), ())), preferred_element_type=F32)


def mm(a, b):
    return jnp.dot(a, b, preferred_element_type=F32)


def iota(shape, dim):
    return lax.broadcasted_iota(jnp.int32, shape, dim)


def as_bf16(condition):
    return jnp.where(condition, 1.0, 0.0).astype(BF16)


def kernel(
    q_hbm, k_hbm, v_hbm, kept_hbm,
    wout_ref, rows_ref, vout_ref,
    q_ref, kept_ref, kv, vt, ebuf, s_a, s_b, q_t, oacc, orecv, mrun, st_send, st_recv,
    slot_of, in_block, band, slot_hot, sendbuf, khalo, vext, vsend, vrecv, vstage,
    load_in, load_k, load_v, own_sem, a2a_send, a2a_recv, q_sem, halo_sem, st_sem, o_sem, vote_send, vote_recv,
):
    me = lax.axis_index("tp")
    grp = lax.axis_index("grp")
    side = me % 2
    head = me // 2
    mate = me + 1 - 2 * side

    row, col = me // 4, me % 4

    def peer(rel):
        return ((row + rel // 4) % 4) * 4 + (col + rel % 4) % 4

    def source(rel):
        return ((row + 4 - rel // 4) % 4) * 4 + (col + 4 - rel % 4) % 4

    def remote(src, dst, send, recv, to):
        return pltpu.make_async_remote_copy(
            src_ref=src, dst_ref=dst, send_sem=send, recv_sem=recv, device_id=(grp, to), device_id_type=MESH
        )

    def k_load(k):
        return pltpu.make_async_copy(k_hbm.at[k], kv.at[:, k, :, pl.ds(0, 128)], load_k.at[k])

    def v_load(k):
        return pltpu.make_async_copy(v_hbm.at[k], kv.at[:, k, :, pl.ds(128, 128)], load_v.at[k])

    barrier = pltpu.get_barrier_semaphore()
    for rel in range(1, OWNERS):
        pl.semaphore_signal(barrier, inc=1, device_id=(grp, peer(rel)), device_id_type=MESH)
    kept_load = pltpu.make_async_copy(kept_hbm, kept_ref, load_in.at[0])
    q_load = pltpu.make_async_copy(q_hbm, q_ref, load_in.at[1])
    kept_load.start()
    q_load.start()
    for k in range(CHUNKS):
        k_load(k).start()
        v_load(k).start()
    kept_load.wait()
    q_load.wait()

    queries = jnp.concatenate([q_ref[:, a * 128 : (a + 1) * 128] for a in range(8)], axis=0)
    q_t[0] = queries.astype(F32).T.astype(BF16)

    mine = jnp.sum(jnp.where(iota((8, 2048), 0) == head, kept_ref[...], 0), axis=0, keepdims=True)
    pos = jnp.where(side == 0, mine[:, :1024], mine[:, 1024:] - HALF)
    blk = pos // BLOCK
    lane = pos % BLOCK
    hot_block = as_bf16(iota((128, 1024), 0) == blk)
    hot_lane = as_bf16(iota((128, 1024), 0) == lane)
    in_block[...] = hot_block
    away = iota((384, 1024), 0) - 128 - lane
    band[...] = as_bf16((away <= 3) & (away >= -3))
    mask = contract_last(hot_block, hot_lane)
    mask16 = mask.astype(BF16)
    r, c = iota((128, 128), 0), iota((128, 128), 1)
    before = mm(mask16, as_bf16(r < c))
    same = mm(as_bf16((c < r) & ((r - c) % OWNERS == 0)), mask16).astype(BF16)
    ahead = mm(same, jnp.ones((128, 128), BF16))
    slots = jnp.where(mask > 0.5, before + ahead, -1.0)
    slot_of[...] = slots
    picked = mm(slots.astype(BF16), hot_lane)
    slot_i = jnp.sum(jnp.where(hot_block > 0.5, picked, 0.0), axis=0, keepdims=True)
    slot_hot[...] = as_bf16(iota((128, 1024), 0).astype(F32) == slot_i)

    window_of = iota((WIN, ROWS), 1) % WIN
    hidden_row = iota((WIN, ROWS), 0) > window_of
    oacc[...] = jnp.zeros_like(oacc)

    def piece_scores(j, k, group, s_ref, top):
        keys = kv[2 * j : 2 * j + 2, k, :, 0:128].reshape(PIECE, 128)
        s = mm(keys, q_t[group])
        if j == PIECES - 1:
            hide = jnp.logical_and(hidden_row, jnp.logical_and(side == 1, k == CHUNKS - 1))
            s = jnp.concatenate([s[: PIECE - WIN], jnp.where(hide, MASKED, s[PIECE - WIN :])], axis=0)
        s_ref[PIECE * j : PIECE * (j + 1), :] = s
        best = jnp.max(s.reshape(PIECE // 8, 8, ROWS), axis=0)
        return best if top is None else jnp.maximum(top, best)

    def scores(k, group, s_ref):
        top = None
        for j in range(PIECES):
            top = piece_scores(j, k, group, s_ref, top)
        return jnp.max(top, axis=0, keepdims=True)

    def transpose_values(k):
        for o in range(OWNERS):
            vt[k, 0:128, o * 128 : (o + 1) * 128] = kv[o, k, :, 128:256].T
        vt[k, 128:144, :] = jnp.ones((16, CHUNK), BF16)

    def advance(k, group, s_ref, old, new, k_next, s_next, group_next):
        u = group * CHUNKS + k
        shift = jnp.broadcast_to(new * SCALE, (8, ROWS))
        top = None
        out = None
        for j in range(PIECES):
            if group_next is not None:
                top = piece_scores(j, k_next, group_next, s_next, top)
            span = slice(PIECE * j, PIECE * (j + 1))
            s = s_ref[span, :].reshape(PIECE // 8, 8, ROWS)
            e = jnp.exp2(s * SCALE - shift[None]).reshape(PIECE, ROWS).astype(BF16)
            ebuf[u, span, :] = e
            part = mm(vt[k, :, span], e)
            out = part if out is None else out + part
        alpha = jnp.exp2((old - new) * SCALE)
        mrun[u] = jnp.broadcast_to(new, (8, ROWS))
        oacc[group] = oacc[group] * alpha + out
        return None if top is None else jnp.max(top, axis=0, keepdims=True)

    def ready(k):
        k_load(k).wait()
        v_load(k).wait()

    lowest = jnp.full((1, ROWS), MASKED, F32)

    def step(group, t, carry, load, follow):
        m_old, mx = carry
        k0, k1 = 2 * t, 2 * t + 1
        if load:
            ready(k1)
        if group == 0:
            transpose_values(k0)
            transpose_values(k1)
        m_new = jnp.maximum(m_old, mx)
        mx1 = advance(k0, group, s_a, m_old, m_new, k1, s_b, group)
        m_last = jnp.maximum(m_new, mx1)
        if load:
            ready(k0 + 2)
        k2 = k0 + 2 if follow == group else 0
        mx2 = advance(k1, group, s_b, m_new, m_last, k2, s_a, follow)
        return m_last, mx2

    def attend(group, first, last, carry):
        return lax.fori_loop(first, last, lambda t, c: step(group, t, c, False, group), carry)

    def finish(group, m):
        st_send[group, 0:8, :] = jnp.broadcast_to(m, (8, ROWS))
        st_send[group, 8:16, :] = oacc[group, 128:136, :]

    def row_copy(rel):
        o = peer(rel)
        return remote(
            sendbuf.at[o],
            rows_ref.at[:, head, pl.ds(side * 128, 128), :],
            a2a_send.at[rel],
            a2a_recv.at[rel],
            o,
        )

    def pick(rel, unused):
        o = peer(rel)
        slot_row = iota((128, 128), 0).astype(F32)
        hot = jnp.concatenate(
            [as_bf16(slot_row == slot_of[pl.ds(16 * k + o, 1), :]) for k in range(CHUNKS)], axis=1
        )
        rows = mm(hot, kv[o].reshape(CHUNKS * 128, 256)).astype(BF16)
        sendbuf[o, 0] = rows[:, 0:128]
        sendbuf[o, 1] = rows[:, 128:256]
        return unused

    def pick_four(t, unused):
        for n in range(4):
            pick(4 * t + n, 0)
        return unused

    ready(0)
    carry = step(0, 0, (lowest, scores(0, 0, s_a)), True, 0)
    waited = 2 * SPLIT
    for k in range(waited + 1, CHUNKS):
        ready(k)
    lax.fori_loop(0, 4, pick_four, 0)
    pl.semaphore_wait(barrier, OWNERS - 1)
    q_copy = remote(q_t.at[0], q_t.at[1], q_sem.at[0], q_sem.at[1], mate)
    q_copy.start()
    edge_owner = 15 - 15 * side
    edge_chunk = 7 - 7 * side
    halo_copy = remote(
        kv.at[edge_owner, edge_chunk, :, pl.ds(0, 128)], khalo, halo_sem.at[0], halo_sem.at[1], mate
    )
    halo_copy.start()
    for rel in EARLY:
        row_copy(rel).start()

    carry = attend(0, SPLIT, CHUNKS // 2 - 1, carry)
    q_copy.wait()
    m_own, mx = step(0, CHUNKS // 2 - 1, carry, False, 1)
    finish(0, m_own)
    own_stat = remote(st_send.at[0], st_recv.at[0], st_sem.at[0], st_sem.at[1], mate)
    carry = attend(1, 0, CHUNKS // 2 - 1, (lowest, mx))
    own_stat.start()
    m_mate, unused = step(1, CHUNKS // 2 - 1, carry, False, None)
    finish(1, m_mate)
    mate_stat = remote(st_send.at[1], st_recv.at[1], st_sem.at[2], st_sem.at[3], mate)
    mate_stat.start()
    out_copy = remote(oacc.at[1], orecv, o_sem.at[0], o_sem.at[1], mate)
    out_copy.start()
    for rel in LATE:
        row_copy(rel).start()
    halo_copy.wait()
    s_halo = [mm(khalo[...], q_t[group]) for group in range(2)]
    own_stat.wait()
    mate_stat.wait()

    m_here = (m_own, m_mate)
    merged = []
    for group in range(2):
        m_there = st_recv[1 - group, 0:1, :]
        l_there = st_recv[1 - group, 8:9, :]
        m_all = jnp.maximum(m_here[group], m_there)
        here = jnp.exp2((m_here[group] - m_all) * SCALE)
        there = jnp.exp2((m_there - m_all) * SCALE)
        l_all = st_send[group, 8:9, :] * here + l_there * there
        merged.append((m_all, here, there, 1.0 / l_all))

    ones = jnp.ones((16, 128), BF16)

    def spread_rows(w):
        return jnp.broadcast_to(w, (16, ROWS)).astype(BF16)[None]

    def fold(parts):
        total = None
        for e, w in parts:
            product = e.reshape(e.shape[0] // 16, 16, ROWS) * w
            both = product[:, :, 0:128] + product[:, :, 128:256]
            total = both if total is None else total + both
        return contract_last(ones, total.reshape(-1, 128))[0:1, :]

    def tally(k, unused):
        parts = []
        for group in range(2):
            m_all, here, there, inv = merged[group]
            u = group * CHUNKS + k
            parts.append((ebuf[u], spread_rows(jnp.exp2((mrun[u, 0:1, :] - m_all) * SCALE) * inv)))
        row = fold(parts)
        for o in range(OWNERS):
            vext[pl.ds(8 + 16 * k + o, 1), :] = row[:, o * 128 : (o + 1) * 128]
        return unused

    def tally_four(t, unused):
        for n in range(4):
            tally(4 * t + n, 0)
        return unused

    lax.fori_loop(0, CHUNKS // 4, tally_four, 0)
    parts = []
    for group in range(2):
        m_all, here, there, inv = merged[group]
        parts.append((jnp.exp2(s_halo[group] * SCALE - m_all * SCALE).astype(BF16), spread_rows(inv)))
    halo_row = fold(parts)
    vext[7:8, :] = jnp.where(side == 1, halo_row, 0.0)
    vext[136:137, :] = jnp.where(side == 0, halo_row, 0.0)
    cut = jnp.logical_and(iota((1, 128), 1) >= 128 - WIN, side == 1)
    vext[135:136, :] = jnp.where(cut, 0.0, vext[135:136, :])

    spread = jnp.concatenate([vext[7:135, :], vext[8:136, :], vext[9:137, :]], axis=1)
    hi = spread.astype(BF16)
    lo = (spread - hi.astype(F32)).astype(BF16)
    pooled = mm(hi, band[...]) + mm(lo, band[...])
    value = jnp.sum(jnp.where(in_block[...] > 0.5, pooled, 0.0), axis=0, keepdims=True) * FACTOR
    by_owner = jnp.where(iota((16, 1024), 0) == blk % OWNERS, value, 0.0).astype(BF16)
    placed = contract_last(by_owner, slot_hot[...])
    for o in range(OWNERS):
        vsend[o] = jnp.broadcast_to(placed[o : o + 1, :], (8, 128))

    def vote_copy(rel):
        return remote(vsend.at[peer(rel)], vrecv.at[me], vote_send.at[rel], vote_recv.at[rel], peer(rel))

    for rel in range(1, OWNERS):
        vote_copy(rel).start()
    vrecv[me] = vsend[me]
    for n in range(2):
        rows_ref[n, head, pl.ds(side * 128, 128), :] = sendbuf[me, n]

    out_copy.wait()
    m_all, here, there, inv = merged[0]
    merged_out = (oacc[0, 0:128, :] * here + orecv[0:128, :] * there) * inv
    by_row = merged_out.T.astype(BF16)
    for a in range(8):
        wout_ref[:, a * 128 : (a + 1) * 128] = by_row[a * WIN : (a + 1) * WIN, :]

    for rel in range(1, OWNERS):
        row_copy(rel).wait()
    for rel in range(1, OWNERS):
        remote(
            vsend.at[peer(rel)], vrecv.at[source(rel)], vote_send.at[rel], vote_recv.at[rel], peer(rel)
        ).wait()
    for t in range(OWNERS):
        vstage[t // 2 : t // 2 + 1, (t % 2) * 128 : (t % 2) * 128 + 128] = vrecv[t, 0:1, :]
    vout_ref[...] = vstage[...].astype(BF16)


def write_out(wout, rows, votes, wout_hbm, kk_hbm, vv_hbm, votes_hbm, sems):
    pairs = ((rows.at[0], kk_hbm), (rows.at[1], vv_hbm), (wout, wout_hbm), (votes, votes_hbm))
    copies = [pltpu.make_async_copy(src, dst, sems.at[n]) for n, (src, dst) in enumerate(pairs)]
    for copy in copies:
        copy.start()
    for copy in copies:
        copy.wait()


def on_device(window_queries, key_rows, value_rows, kept):
    vmem = pl.BlockSpec(memory_space=pltpu.VMEM)
    hbm = pl.BlockSpec(memory_space=pltpu.HBM)
    dma = pltpu.SemaphoreType.DMA
    shaped = (CHUNKS, OWNERS, BLOCK, 128)
    inside = pl.pallas_call(
        kernel,
        out_shape=(
            pltpu.VMEM((WIN, 1024), BF16),
            pltpu.VMEM((2, 8, 256, 128), BF16),
            pltpu.VMEM((8, 256), BF16),
        ),
        in_specs=[hbm] * 4,
        out_specs=(vmem,) * 3,
        scratch_shapes=[
            pltpu.VMEM((WIN, 1024), BF16),
            pltpu.VMEM((8, 2048), jnp.int32),
            pltpu.VMEM((OWNERS, CHUNKS, BLOCK, 256), BF16),
            pltpu.VMEM((CHUNKS, 144, CHUNK), BF16),
            pltpu.VMEM((2 * CHUNKS, CHUNK, ROWS), BF16),
            pltpu.VMEM((CHUNK, ROWS), F32),
            pltpu.VMEM((CHUNK, ROWS), F32),
            pltpu.VMEM((2, 128, ROWS), BF16),
            pltpu.VMEM((2, 144, ROWS), F32),
            pltpu.VMEM((144, ROWS), F32),
            pltpu.VMEM((2 * CHUNKS, 8, ROWS), F32),
            pltpu.VMEM((2, 16, ROWS), F32),
            pltpu.VMEM((2, 16, ROWS), F32),
            pltpu.VMEM((128, 128), F32),
            pltpu.VMEM((128, 1024), BF16),
            pltpu.VMEM((384, 1024), BF16),
            pltpu.VMEM((128, 1024), BF16),
            pltpu.VMEM((OWNERS, 2, 128, 128), BF16),
            pltpu.VMEM((128, 128), BF16),
            pltpu.VMEM((144, 128), F32),
            pltpu.VMEM((OWNERS, 8, 128), F32),
            pltpu.VMEM((OWNERS, 8, 128), F32),
            pltpu.VMEM((8, 256), F32),
            dma((2,)),
            dma((CHUNKS,)),
            dma((CHUNKS,)),
            dma((2,)),
            dma((OWNERS,)),
            dma((OWNERS,)),
            dma((2,)),
            dma((2,)),
            dma((4,)),
            dma((2,)),
            dma((OWNERS,)),
            dma((OWNERS,)),
        ],
        compiler_params=pltpu.CompilerParams(
            collective_id=0, has_side_effects=True, vmem_limit_bytes=56 * 1024 * 1024
        ),
    )(window_queries, key_rows.reshape(shaped), value_rows.reshape(shaped), kept)
    wout, kk, vv, votes = pl.pallas_call(
        write_out,
        out_shape=(
            jax.ShapeDtypeStruct((WIN, 1024), BF16),
            jax.ShapeDtypeStruct((8, 256, 128), BF16),
            jax.ShapeDtypeStruct((8, 256, 128), BF16),
            jax.ShapeDtypeStruct((8, 256), BF16),
        ),
        in_specs=[vmem] * 3,
        out_specs=(hbm,) * 4,
        scratch_shapes=[dma((4,))],
        compiler_params=pltpu.CompilerParams(vmem_limit_bytes=1024 * 1024),
    )(*inside)
    return (wout, kk[None], vv[None], votes[None])


def solution(mesh):
    return jax.shard_map(
        on_device,
        mesh=mesh,
        in_specs=(P("grp", "tp"), P("tp", "grp", None), P("tp", "grp", None), P(None, "grp")),
        out_specs=(
            P("grp", "tp"),
            P("tp", None, "grp", None),
            P("tp", None, "grp", None),
            P("tp", "grp", None),
        ),
        check_vma=False,
    )
```

```python
import functools

import jax
import jax.numpy as jnp
from jax import lax
from jax.experimental import pallas as pl
from jax.experimental.pallas import tpu as pltpu
from jax.sharding import PartitionSpec as P

SEQ = 32768
WIN = 32
HALF = 16384
EARLY = (2, 4, 1, 3, 8, 6, 5, 7, 12, 10, 9, 11)
LATE = (14, 13, 15)
CHUNKS = 8
OWNERS = 16
BLOCK = 128
ROWS = 256
CHUNK = OWNERS * BLOCK
PIECE = 256
PIECES = CHUNK // PIECE
SCALE = 1.4426950408889634 / 128.0**0.5
FACTOR = (SEQ - WIN) / (7.0 * 16 * WIN)
MASKED = -1e30
F32 = jnp.float32
BF16 = jnp.bfloat16
MESH = pl.DeviceIdType.MESH


def contract_last(a, b):
    return lax.dot_general(a, b, (((1,), (1,)), ((), ())), preferred_element_type=F32)


def mm(a, b):
    return jnp.dot(a, b, preferred_element_type=F32)


def iota(shape, dim):
    return lax.broadcasted_iota(jnp.int32, shape, dim)


def as_bf16(condition):
    return jnp.where(condition, 1.0, 0.0).astype(BF16)


def kernel(
    q_hbm, k_hbm, v_hbm, kept_hbm,
    wout_ref, rows_ref, vout_ref,
    q_ref, kept_ref, kv, vt, ebuf, s_a, s_b, q_t, oacc, orecv, mrun, st_send, st_recv,
    slot_of, in_block, band, slot_hot, sendbuf, khalo, vext, vsend, vrecv, vstage,
    load_in, load_k, load_v, own_sem, a2a_send, a2a_recv, q_sem, halo_sem, st_sem, o_sem, vote_send, vote_recv,
):
    me = lax.axis_index("tp")
    grp = lax.axis_index("grp")
    side = me % 2
    head = me // 2
    mate = me + 1 - 2 * side

    row, col = me // 4, me % 4

    def peer(rel):
        return ((row + rel // 4) % 4) * 4 + (col + rel % 4) % 4

    def source(rel):
        return ((row + 4 - rel // 4) % 4) * 4 + (col + 4 - rel % 4) % 4

    def remote(src, dst, send, recv, to):
        return pltpu.make_async_remote_copy(
            src_ref=src, dst_ref=dst, send_sem=send, recv_sem=recv, device_id=(grp, to), device_id_type=MESH
        )

    def k_load(k):
        return pltpu.make_async_copy(k_hbm.at[k], kv.at[:, k, :, pl.ds(0, 128)], load_k.at[k])

    def v_load(k):
        return pltpu.make_async_copy(v_hbm.at[k], kv.at[:, k, :, pl.ds(128, 128)], load_v.at[k])

    khalo[...] = jnp.zeros_like(khalo)
    barrier = pltpu.get_barrier_semaphore()
    for rel in range(1, OWNERS):
        pl.semaphore_signal(barrier, inc=1, device_id=(grp, peer(rel)), device_id_type=MESH)
    kept_load = pltpu.make_async_copy(kept_hbm, kept_ref, load_in.at[0])
    q_load = pltpu.make_async_copy(q_hbm, q_ref, load_in.at[1])
    kept_load.start()
    q_load.start()
    for k in range(CHUNKS):
        k_load(k).start()
        v_load(k).start()
    kept_load.wait()
    q_load.wait()

    queries = jnp.concatenate([q_ref[:, a * 128 : (a + 1) * 128] for a in range(8)], axis=0)
    q_t[0] = queries.astype(F32).T.astype(BF16)

    mine = jnp.sum(jnp.where(iota((8, 2048), 0) == head, kept_ref[...], 0), axis=0, keepdims=True)
    pos = jnp.where(side == 0, mine[:, :1024], mine[:, 1024:] - HALF)
    blk = pos // BLOCK
    lane = pos % BLOCK
    hot_block = as_bf16(iota((128, 1024), 0) == blk)
    hot_lane = as_bf16(iota((128, 1024), 0) == lane)
    in_block[...] = hot_block
    away = iota((384, 1024), 0) - 128 - lane
    band[...] = as_bf16((away <= 3) & (away >= -3))
    mask = contract_last(hot_block, hot_lane)
    mask16 = mask.astype(BF16)
    r, c = iota((128, 128), 0), iota((128, 128), 1)
    before = mm(mask16, as_bf16(r < c))
    same = mm(as_bf16((c < r) & ((r - c) % OWNERS == 0)), mask16).astype(BF16)
    ahead = mm(same, jnp.ones((128, 128), BF16))
    slots = jnp.where(mask > 0.5, before + ahead, -1.0)
    slot_of[...] = slots
    picked = mm(slots.astype(BF16), hot_lane)
    slot_i = jnp.sum(jnp.where(hot_block > 0.5, picked, 0.0), axis=0, keepdims=True)
    slot_hot[...] = as_bf16(iota((128, 1024), 0).astype(F32) == slot_i)

    window_of = iota((WIN, ROWS), 1) % WIN
    hidden_row = iota((WIN, ROWS), 0) > window_of
    oacc[...] = jnp.zeros_like(oacc)

    def piece_scores(j, k, group, s_ref, top):
        keys = kv[2 * j : 2 * j + 2, k, :, 0:128].reshape(PIECE, 128)
        s = mm(keys, q_t[group])
        if j == PIECES - 1:
            hide = jnp.logical_and(hidden_row, jnp.logical_and(side == 1, k == CHUNKS - 1))
            s = jnp.concatenate([s[: PIECE - WIN], jnp.where(hide, MASKED, s[PIECE - WIN :])], axis=0)
        s_ref[PIECE * j : PIECE * (j + 1), :] = s
        best = jnp.max(s.reshape(PIECE // 8, 8, ROWS), axis=0)
        return best if top is None else jnp.maximum(top, best)

    def scores(k, group, s_ref):
        top = None
        for j in range(PIECES):
            top = piece_scores(j, k, group, s_ref, top)
        return jnp.max(top, axis=0, keepdims=True)

    def transpose_values(k):
        for o in range(OWNERS):
            vt[k, 0:128, o * 128 : (o + 1) * 128] = kv[o, k, :, 128:256].T
        vt[k, 128:144, :] = jnp.ones((16, CHUNK), BF16)

    def advance(k, group, s_ref, old, new, k_next, s_next, group_next):
        u = group * CHUNKS + k
        shift = jnp.broadcast_to(new * SCALE, (8, ROWS))
        top = None
        out = None
        for j in range(PIECES):
            if group_next is not None:
                top = piece_scores(j, k_next, group_next, s_next, top)
            span = slice(PIECE * j, PIECE * (j + 1))
            s = s_ref[span, :].reshape(PIECE // 8, 8, ROWS)
            e = jnp.exp2(s * SCALE - shift[None]).reshape(PIECE, ROWS).astype(BF16)
            ebuf[u, span, :] = e
            part = mm(vt[k, :, span], e)
            out = part if out is None else out + part
        alpha = jnp.exp2((old - new) * SCALE)
        mrun[u] = jnp.broadcast_to(new, (8, ROWS))
        oacc[group] = oacc[group] * alpha + out
        return None if top is None else jnp.max(top, axis=0, keepdims=True)

    def ready(k):
        k_load(k).wait()
        v_load(k).wait()

    lowest = jnp.full((1, ROWS), MASKED, F32)

    def step(group, t, carry, follow):
        m_old, mx = carry
        k0, k1 = 2 * t, 2 * t + 1
        if group == 0:
            transpose_values(k0)
            transpose_values(k1)
        m_new = jnp.maximum(m_old, mx)
        mx1 = advance(k0, group, s_a, m_old, m_new, k1, s_b, group)
        m_last = jnp.maximum(m_new, mx1)
        k2 = k0 + 2 if follow == group else 0
        mx2 = advance(k1, group, s_b, m_new, m_last, k2, s_a, follow)
        return m_last, mx2

    def attend(group, first, last, carry):
        return lax.fori_loop(first, last, lambda t, c: step(group, t, c, group), carry)

    def finish(group, m):
        st_send[group, 0:8, :] = jnp.broadcast_to(m, (8, ROWS))
        st_send[group, 8:16, :] = oacc[group, 128:136, :]

    def row_copy(rel):
        o = peer(rel)
        return remote(
            sendbuf.at[o],
            rows_ref.at[:, head, pl.ds(side * 128, 128), :],
            a2a_send.at[rel],
            a2a_recv.at[rel],
            o,
        )

    def pick(rel, unused):
        o = peer(rel)
        slot_row = iota((128, 128), 0).astype(F32)
        hot = jnp.concatenate(
            [as_bf16(slot_row == slot_of[pl.ds(16 * k + o, 1), :]) for k in range(CHUNKS)], axis=1
        )
        rows = mm(hot, kv[o].reshape(CHUNKS * 128, 256)).astype(BF16)
        sendbuf[o, 0] = rows[:, 0:128]
        sendbuf[o, 1] = rows[:, 128:256]
        return unused

    def pick_four(t, unused):
        for n in range(4):
            pick(4 * t + n, 0)
        return unused

    ready(0)
    first = scores(0, 0, s_a)
    for k in range(1, CHUNKS):
        ready(k)
    lax.fori_loop(0, 4, pick_four, 0)
    pl.semaphore_wait(barrier, OWNERS - 1)
    q_copy = remote(q_t.at[0], q_t.at[1], q_sem.at[0], q_sem.at[1], mate)
    q_copy.start()
    edge_owner = 15 - 15 * side
    edge_chunk = 7 - 7 * side
    edge_row = 112 - 112 * side

    def halo(to_row):
        return remote(
            kv.at[edge_owner, edge_chunk, pl.ds(edge_row, 16), pl.ds(0, 128)],
            khalo.at[pl.ds(to_row, 16), :],
            halo_sem.at[0],
            halo_sem.at[1],
            mate,
        )

    halo(edge_row).start()
    for rel in EARLY:
        row_copy(rel).start()

    carry = attend(0, 0, CHUNKS // 2 - 1, (lowest, first))
    q_copy.wait()
    m_own, mx = step(0, CHUNKS // 2 - 1, carry, 1)
    finish(0, m_own)
    own_stat = remote(st_send.at[0], st_recv.at[0], st_sem.at[0], st_sem.at[1], mate)
    carry = attend(1, 0, CHUNKS // 2 - 1, (lowest, mx))
    own_stat.start()
    m_mate, unused = step(1, CHUNKS // 2 - 1, carry, None)
    finish(1, m_mate)
    mate_stat = remote(st_send.at[1], st_recv.at[1], st_sem.at[2], st_sem.at[3], mate)
    mate_stat.start()
    out_copy = remote(oacc.at[1, pl.ds(0, 128), :], orecv, o_sem.at[0], o_sem.at[1], mate)
    out_copy.start()
    for rel in LATE:
        row_copy(rel).start()
    halo(112 * side).wait()
    s_halo = [mm(khalo[...], q_t[group]) for group in range(2)]
    own_stat.wait()
    mate_stat.wait()

    m_here = (m_own, m_mate)
    merged = []
    for group in range(2):
        m_there = st_recv[1 - group, 0:1, :]
        l_there = st_recv[1 - group, 8:9, :]
        m_all = jnp.maximum(m_here[group], m_there)
        here = jnp.exp2((m_here[group] - m_all) * SCALE)
        there = jnp.exp2((m_there - m_all) * SCALE)
        l_all = st_send[group, 8:9, :] * here + l_there * there
        merged.append((m_all, here, there, 1.0 / l_all))

    ones = jnp.ones((16, 128), BF16)

    def spread_rows(w):
        return jnp.broadcast_to(w, (16, ROWS)).astype(BF16)[None]

    def fold(parts):
        total = None
        for e, w in parts:
            product = e.reshape(e.shape[0] // 16, 16, ROWS) * w
            both = product[:, :, 0:128] + product[:, :, 128:256]
            total = both if total is None else total + both
        return contract_last(ones, total.reshape(-1, 128))[0:1, :]

    def tally(k, unused):
        parts = []
        for group in range(2):
            m_all, here, there, inv = merged[group]
            u = group * CHUNKS + k
            parts.append((ebuf[u], spread_rows(jnp.exp2((mrun[u, 0:1, :] - m_all) * SCALE) * inv)))
        row = fold(parts)
        for o in range(OWNERS):
            vext[pl.ds(8 + 16 * k + o, 1), :] = row[:, o * 128 : (o + 1) * 128]
        return unused

    def tally_four(t, unused):
        for n in range(4):
            tally(4 * t + n, 0)
        return unused

    lax.fori_loop(0, CHUNKS // 4, tally_four, 0)
    parts = []
    for group in range(2):
        m_all, here, there, inv = merged[group]
        parts.append((jnp.exp2(s_halo[group] * SCALE - m_all * SCALE).astype(BF16), spread_rows(inv)))
    halo_row = fold(parts)
    along = iota((1, 128), 1)
    vext[7:8, :] = jnp.where(jnp.logical_and(side == 1, along >= 125), halo_row, 0.0)
    vext[136:137, :] = jnp.where(jnp.logical_and(side == 0, along < 3), halo_row, 0.0)
    cut = jnp.logical_and(iota((1, 128), 1) >= 128 - WIN, side == 1)
    vext[135:136, :] = jnp.where(cut, 0.0, vext[135:136, :])

    spread = jnp.concatenate([vext[7:135, :], vext[8:136, :], vext[9:137, :]], axis=1)
    hi = spread.astype(BF16)
    lo = (spread - hi.astype(F32)).astype(BF16)
    pooled = mm(hi, band[...]) + mm(lo, band[...])
    value = jnp.sum(jnp.where(in_block[...] > 0.5, pooled, 0.0), axis=0, keepdims=True) * FACTOR
    by_owner = jnp.where(iota((16, 1024), 0) == blk % OWNERS, value, 0.0).astype(BF16)
    placed = contract_last(by_owner, slot_hot[...])
    for o in range(OWNERS):
        vsend[o] = jnp.broadcast_to(placed[o : o + 1, :], (8, 128))

    def vote_copy(rel):
        return remote(vsend.at[peer(rel)], vrecv.at[me], vote_send.at[rel], vote_recv.at[rel], peer(rel))

    for rel in range(1, OWNERS):
        vote_copy(rel).start()
    vrecv[me] = vsend[me]
    for n in range(2):
        rows_ref[n, head, pl.ds(side * 128, 128), :] = sendbuf[me, n]

    out_copy.wait()
    m_all, here, there, inv = merged[0]
    merged_out = (oacc[0, 0:128, :] * here + orecv[...] * there) * inv
    by_row = merged_out.T.astype(BF16)
    for a in range(8):
        wout_ref[:, a * 128 : (a + 1) * 128] = by_row[a * WIN : (a + 1) * WIN, :]

    for rel in range(1, OWNERS):
        row_copy(rel).wait()
    for rel in range(1, OWNERS):
        remote(
            vsend.at[peer(rel)], vrecv.at[source(rel)], vote_send.at[rel], vote_recv.at[rel], peer(rel)
        ).wait()
    for t in range(OWNERS):
        vstage[t // 2 : t // 2 + 1, (t % 2) * 128 : (t % 2) * 128 + 128] = vrecv[t, 0:1, :]
    vout_ref[...] = vstage[...].astype(BF16)


def write_out(wout, rows, votes, wout_hbm, kk_hbm, vv_hbm, votes_hbm, sems):
    pairs = ((rows.at[0], kk_hbm), (rows.at[1], vv_hbm), (wout, wout_hbm), (votes, votes_hbm))
    copies = [pltpu.make_async_copy(src, dst, sems.at[n]) for n, (src, dst) in enumerate(pairs)]
    for copy in copies:
        copy.start()
    for copy in copies:
        copy.wait()


def on_device(window_queries, key_rows, value_rows, kept):
    vmem = pl.BlockSpec(memory_space=pltpu.VMEM)
    hbm = pl.BlockSpec(memory_space=pltpu.HBM)
    dma = pltpu.SemaphoreType.DMA
    shaped = (CHUNKS, OWNERS, BLOCK, 128)
    inside = pl.pallas_call(
        kernel,
        out_shape=(
            pltpu.VMEM((WIN, 1024), BF16),
            pltpu.VMEM((2, 8, 256, 128), BF16),
            pltpu.VMEM((8, 256), BF16),
        ),
        in_specs=[hbm] * 4,
        out_specs=(vmem,) * 3,
        scratch_shapes=[
            pltpu.VMEM((WIN, 1024), BF16),
            pltpu.VMEM((8, 2048), jnp.int32),
            pltpu.VMEM((OWNERS, CHUNKS, BLOCK, 256), BF16),
            pltpu.VMEM((CHUNKS, 144, CHUNK), BF16),
            pltpu.VMEM((2 * CHUNKS, CHUNK, ROWS), BF16),
            pltpu.VMEM((CHUNK, ROWS), F32),
            pltpu.VMEM((CHUNK, ROWS), F32),
            pltpu.VMEM((2, 128, ROWS), BF16),
            pltpu.VMEM((2, 144, ROWS), F32),
            pltpu.VMEM((128, ROWS), F32),
            pltpu.VMEM((2 * CHUNKS, 8, ROWS), F32),
            pltpu.VMEM((2, 16, ROWS), F32),
            pltpu.VMEM((2, 16, ROWS), F32),
            pltpu.VMEM((128, 128), F32),
            pltpu.VMEM((128, 1024), BF16),
            pltpu.VMEM((384, 1024), BF16),
            pltpu.VMEM((128, 1024), BF16),
            pltpu.VMEM((OWNERS, 2, 128, 128), BF16),
            pltpu.VMEM((128, 128), BF16),
            pltpu.VMEM((144, 128), F32),
            pltpu.VMEM((OWNERS, 8, 128), F32),
            pltpu.VMEM((OWNERS, 8, 128), F32),
            pltpu.VMEM((8, 256), F32),
            dma((2,)),
            dma((CHUNKS,)),
            dma((CHUNKS,)),
            dma((2,)),
            dma((OWNERS,)),
            dma((OWNERS,)),
            dma((2,)),
            dma((2,)),
            dma((4,)),
            dma((2,)),
            dma((OWNERS,)),
            dma((OWNERS,)),
        ],
        compiler_params=pltpu.CompilerParams(
            collective_id=0, has_side_effects=True, vmem_limit_bytes=56 * 1024 * 1024
        ),
    )(window_queries, key_rows.reshape(shaped), value_rows.reshape(shaped), kept)
    wout, kk, vv, votes = pl.pallas_call(
        write_out,
        out_shape=(
            jax.ShapeDtypeStruct((WIN, 1024), BF16),
            jax.ShapeDtypeStruct((8, 256, 128), BF16),
            jax.ShapeDtypeStruct((8, 256, 128), BF16),
            jax.ShapeDtypeStruct((8, 256), BF16),
        ),
        in_specs=[vmem] * 3,
        out_specs=(hbm,) * 4,
        scratch_shapes=[dma((4,))],
        compiler_params=pltpu.CompilerParams(vmem_limit_bytes=1024 * 1024),
    )(*inside)
    return (wout, kk[None], vv[None], votes[None])


def solution(mesh):
    return jax.shard_map(
        on_device,
        mesh=mesh,
        in_specs=(P("grp", "tp"), P("tp", "grp", None), P("tp", "grp", None), P(None, "grp")),
        out_specs=(
            P("grp", "tp"),
            P("tp", None, "grp", None),
            P("tp", None, "grp", None),
            P("tp", "grp", None),
        ),
        check_vma=False,
    )
```
